32 devices in a mesh: rows: 8 (over z, y), dp: 4 (over x, core).
Axes of the slice: x: 2, y: 2, z: 4, core: 2. Of those that a mesh axis runs over, the one named last changes fastest.
Arguments:
- weights: float32 [6144, 4096], P(('rows', 'dp'))
- moment: float32 [6144, 4096], P(('rows', 'dp'))
- second: float32 [6144, 4096], P(('rows', 'dp')), may hold values from 0.01 to 1
- tile_rows: bfloat16 [2048, 4096], P(('rows', 'dp')), may hold values from -6 to 6
- row_index: int32 [2048], P(('rows', 'dp')), may hold values from 0 to 191
- bucket_count: int32 [1024], P(('rows', 'dp')), may hold values from 1 to 2, as said below
Outputs:
- new_weights: float32 [6144, 4096], P(('rows', 'dp'))
- new_moment: float32 [6144, 4096], P(('rows', 'dp'))
- new_second: float32 [6144, 4096], P(('rows', 'dp'))
The draws below stay inside these ranges and needn't reach their ends.
Inputs may be any that keep to these rules, and one draw needn't show every extreme that they name: `bucket_count`: at least one slot of every sender and owner is live; in every draw some owner receives 2 live slots from every sender. `row_index`: rows may repeat within and across senders.
All inputs are finite; a program needn't handle non-finite values.
Results may differ from the reference program's by a relative error of at most 0.0003.
Values may be sent and summed in bfloat16 or wider, within the bound.
A program may use at most 64 MiB of HBM per device.

```python
import math
import jax
import jax.numpy as jnp

D = 4096
ROWS_DEV = 192
CAP = 2
OWNERS = 32
VOCAB = 6144
SLOTS = 64


def draw_weights(key, part):
    key_one = jax.random.fold_in(key, 21)
    key_two = jax.random.fold_in(key, 22)
    key_three = jax.random.fold_in(key, 23)
    row_pos = jnp.arange(VOCAB, dtype=jnp.float32) / VOCAB
    normal_part = jax.random.truncated_normal(key_one, -4.0, 4.0, (VOCAB, D), jnp.float32)
    row_scale = 10.0 ** jax.random.uniform(key_two, (VOCAB, 1), jnp.float32) * 3.0 ** row_pos[:, None]
    col_scale = 10.0 ** jax.random.uniform(key_three, (1, D), jnp.float32)
    return 0.05 * normal_part * row_scale * col_scale


def draw_moment(key, part):
    key_one = jax.random.fold_in(key, 31)
    key_two = jax.random.fold_in(key, 32)
    row_pos = jnp.arange(VOCAB, dtype=jnp.float32) / VOCAB
    normal_part = jax.random.truncated_normal(key_one, -4.0, 4.0, (VOCAB, D), jnp.float32)
    row_scale = 10.0 ** jax.random.uniform(key_two, (VOCAB, 1), jnp.float32) * 3.0 ** row_pos[:, None]
    return 0.05 * normal_part * row_scale


def draw_bucket_count(key, part):
    key_one = jax.random.fold_in(key, 11)
    key_two = jax.random.fold_in(key, 12)
    counts_all = jax.random.randint(key_one, (OWNERS, OWNERS), 1, CAP + 1)
    full_owner = jax.random.randint(key_two, (), 0, OWNERS)
    column_id = jnp.arange(OWNERS)[None, :]
    return jnp.where(column_id == full_owner, CAP, counts_all).reshape(-1).astype(jnp.int32)


def touch_ends(entries, stream_key, least, largest):
    spot = [jax.random.randint(jax.random.fold_in(stream_key, axis), (), 0, length) for axis, length in enumerate(entries.shape)]
    widest = entries.shape.index(max(entries.shape))
    next_to = spot[:widest] + [(spot[widest] + 1) % entries.shape[widest]] + spot[widest + 1:]
    return entries.at[tuple(spot)].set(least).at[tuple(next_to)].set(largest)


def steps_of(stream_key, extent, split, least, largest):
    factor_of = 1.0
    for dim, shards_of in split:
        steps = jax.random.uniform(jax.random.fold_in(jax.random.fold_in(stream_key, 6), dim), (shards_of,), jnp.float32, least / len(split), largest / len(split))
        factor_of = factor_of * jnp.repeat(jnp.exp(steps), extent[dim] // shards_of).reshape((-1,) + (1,) * (len(extent) - 1 - dim))
    return factor_of


def gaussian(stream_key, extent, scale, limit, shards=(), kind=jnp.bfloat16):
    loudness = steps_of(stream_key, extent, shards, -0.22, 0.18) if shards else 1.0
    array = jax.random.normal(stream_key, extent, jnp.float32) * scale * loudness
    return jnp.minimum(jnp.maximum(array, -limit), limit).astype(kind)


def setup_inputs(seed: int = 0) -> dict:
    streams_of = jax.random.split(jax.random.key(seed), 7)
    return {
        "weights": draw_weights(jax.random.fold_in(streams_of[6], 71), 0),
        "moment": draw_moment(jax.random.fold_in(streams_of[6], 71), 0),
        "second": jnp.clip(jnp.exp(math.log(1.0) - 4.6051702 * jax.random.uniform(streams_of[2], (VOCAB, D), jnp.float32) ** steps_of(streams_of[2], (VOCAB, D), ((0, 32),), -0.2, 0.2)), 0.01, 1.0),
        "tile_rows": gaussian(streams_of[3], (OWNERS * SLOTS, D), 1.0, 6.0, ((0, 32),)),
        "row_index": touch_ends(jax.random.randint(streams_of[4], (OWNERS * SLOTS,), 0, ROWS_DEV), jax.random.fold_in(streams_of[4], 1), 0, ROWS_DEV - 1).astype(jnp.int32),
        "bucket_count": draw_bucket_count(jax.random.fold_in(streams_of[6], 71), 0),
    }


beta_one = 0.9
beta_two = 0.999
epsilon = 1e-06
decay = 0.01
rate = 0.1

def reference(weights, moment, second, tile_rows, row_index, bucket_count):
    position = jnp.arange(OWNERS * SLOTS, dtype=jnp.int32)
    slot_pos = position % CAP
    bucket_id = position // CAP
    owner_id = bucket_id % OWNERS
    is_live = slot_pos < bucket_count[bucket_id]
    table_row = jnp.where(is_live, owner_id * ROWS_DEV + row_index, 0).astype(jnp.int32)
    values = tile_rows.astype(jnp.float32) * is_live.astype(jnp.float32)[:, None]
    gradient = jax.ops.segment_sum(values, table_row, num_segments=VOCAB)
    new_moment = beta_one * moment + (1.0 - beta_one) * gradient
    new_second = beta_two * second + (1.0 - beta_two) * gradient * gradient
    update = new_moment / (jnp.sqrt(new_second) + epsilon) + decay * weights
    weight_sq = jnp.sum(weights * weights)
    update_sq = jnp.sum(update * update)
    trust_ratio = jnp.sqrt(weight_sq) / jnp.sqrt(update_sq + 1e-06)
    new_weights = weights - rate * trust_ratio * update
    return (new_weights, new_moment, new_second)
```

```python
import functools

import jax
import jax.numpy as jnp
from jax import lax
from jax.experimental import pallas as pl
from jax.experimental.pallas import tpu as pltpu
from jax.sharding import PartitionSpec as P

beta_one = 0.9
beta_two = 0.999
epsilon = 1e-06
decay = 0.01
rate = 0.1

AXES = ("rows", "dp")
LANES = 128


def factors(rows, dp):
    lo = max(d for d in range(1, rows + 1) if rows % d == 0 and d * d <= rows)
    core = 2 if dp % 2 == 0 else 1
    return rows // lo, lo, dp // core, core


def pieces_of(groups):
    big = max(groups // 8, 1)
    sizes = [big] * (groups // big)
    while sizes[-1] > 1:
        last = sizes.pop()
        sizes += [last - last // 2, last // 2]
    return sizes


def exchange(
    grid, weights, moment, second, tiles, index, count,
    weight_out, moment_out, second_out, update_out, scale_out,
    staged, landed, index_all, count_all, parts, picker,
    load_sem, stage_sem, own_sem, ready, near_send, near_recv, tile_send, tile_recv,
    line_send, line_recv, plane_send, plane_recv, part_send, part_recv,
):
    Z, L, X, C = grid
    n = Z * L * X * C
    fast = X * C
    columns = L * X * C
    row_id, dp_id = lax.axis_index("rows"), lax.axis_index("dp")
    me = row_id * fast + dp_id
    hi, lo = row_id // L, lax.rem(row_id, L)
    x, core = dp_id // C, lax.rem(dp_id, C)
    column = lo * fast + dp_id
    rows_here, width = weights.shape
    groups = width // LANES
    slots = index.shape[-1]
    capacity = slots // n
    pack = tiles.shape[2]
    sizes = pieces_of(groups)

    half = Z // 2 if Z % 2 == 0 else 0
    if half:
        side = hi // half
        inside = hi - side * half
        line = [side * k + (1 - side) * (Z - 1 - k) for k in range(half)]
        line += [side * half + lax.rem(inside + j, half) for j in range(1, half)]
    else:
        line = [lax.rem(hi + j, Z) for j in range(1, Z)]
    los = [lo] + [lax.rem(lo + j, L) for j in range(1, L)]
    xs = [x] + [lax.rem(x + j, X) for j in range(1, X)]
    cores = [core] + [lax.rem(core + j, C) for j in range(1, C)]

    def spot(h, a, b, c):
        r, d = h * L + a, b * C + c
        return {"rows": r, "dp": d}, r * fast + d

    others = [
        (a, b, c)
        for j, a in list(enumerate(los))[::-1]
        for k, b in list(enumerate(xs))[::-1]
        if j or k
        for c in cores
    ]
    line_peers = [spot(h, lo, x, core) for h in line]
    plane_peers = [spot(hi, a, b, c) for a, b, c in others]
    plane_peers += [spot(hi, lo, x, c) for c in cores[1:]]
    near = [spot(h, lo, x, c) for h in line for c in cores] + plane_peers
    far = [spot(h, a, b, c) for h in line for a, b, c in others]

    def mesh_copy(src, dst, send, recv, where):
        return pltpu.make_async_remote_copy(
            src_ref=src, dst_ref=dst, send_sem=send, recv_sem=recv,
            device_id=where, device_id_type=pl.DeviceIdType.MESH,
        )

    def drain(ref, sem):
        pltpu.make_async_copy(ref, ref, sem).wait()

    stage = [
        pltpu.make_async_copy(tiles, staged, stage_sem.at[0]),
        pltpu.make_async_copy(index, index_all.at[column, hi], stage_sem.at[1]),
        pltpu.make_async_copy(count, count_all.at[column, hi], stage_sem.at[2]),
    ]
    for copy in stage:
        copy.start()
    barrier = pltpu.get_barrier_semaphore()
    for where, _ in near:
        pl.semaphore_signal(
            barrier, inc=1, device_id=where, device_id_type=pl.DeviceIdType.MESH
        )
    own = pltpu.make_async_copy(
        tiles.at[me // pack, :, lax.rem(me, pack)], landed.at[:, me], own_sem
    )
    own.start()
    loads = [
        pltpu.make_async_copy(weights, weight_out, load_sem.at[0]),
        pltpu.make_async_copy(moment, moment_out, load_sem.at[1]),
        pltpu.make_async_copy(second, second_out, load_sem.at[2]),
    ]
    for load in loads:
        load.start()
    for copy in stage:
        copy.wait()
    pl.semaphore_wait(barrier, len(near))

    for where, _ in line_peers:
        pl.semaphore_signal(
            ready, inc=1, device_id=where, device_id_type=pl.DeviceIdType.MESH
        )
    for where, peer in near:
        mesh_copy(
            staged.at[peer // pack, :, lax.rem(peer, pack)], landed.at[:, me],
            near_send, near_recv, where,
        ).start()
    small = (index_all, count_all)
    for k, ref in enumerate(small):
        mine = ref.at[column, hi]
        for where, _ in line_peers:
            mesh_copy(mine, mine, line_send.at[k], line_recv.at[k], where).start()

    if line_peers:
        pl.semaphore_wait(ready, len(line_peers))
    start = 0
    for q, size in enumerate(sizes):
        span = pl.ds(start, size)
        for where, peer in far:
            mesh_copy(
                staged.at[peer // pack, span, lax.rem(peer, pack)],
                landed.at[span, me], tile_send.at[q], tile_recv.at[q], where,
            ).start()
        start += size

    for k, ref in enumerate(small):
        if line_peers:
            drain(ref.at[column, pl.ds(0, Z - 1)], line_recv.at[k])
        block = ref.at[column]
        for where, _ in plane_peers:
            mesh_copy(block, block, plane_send.at[k], plane_recv.at[k], where).start()

    loads[0].wait()

    def weight_step(g, total):
        w = weight_out[:, pl.ds(pl.multiple_of(g * LANES, LANES), LANES)]
        return total + jnp.sum((w * w).reshape(rows_here // 8, 8, LANES), axis=0)

    zero = jnp.zeros((8, LANES), jnp.float32)
    weight_sum = lax.fori_loop(0, groups, weight_step, zero, unroll=4)
    weight_row = jnp.sum(weight_sum, axis=0, keepdims=True)
    weight_row = weight_row + pltpu.roll(weight_row, LANES // 2, 1)

    if plane_peers:
        for k, ref in enumerate(small):
            drain(ref.at[pl.ds(0, columns - 1)], plane_recv.at[k])
    index_rows = jnp.concatenate([index_all[:, h, 0, :] for h in range(Z)], axis=0)
    count_rows = jnp.concatenate([count_all[:, h, 0, :] for h in range(Z)], axis=0)
    lane = lax.broadcasted_iota(jnp.int32, (n, slots), 1)
    order = lax.broadcasted_iota(jnp.int32, (n, slots), 0)
    owner = lax.broadcasted_iota(jnp.int32, (n, n), 1)
    live = jnp.sum(jnp.where(owner == me, count_rows, 0), axis=1, keepdims=True)
    spread = jnp.zeros((n, slots), jnp.int32)
    for c in range(capacity):
        goal = jnp.sum(
            jnp.where(lane == me * capacity + c, index_rows, 0), axis=1, keepdims=True
        )
        goal = jnp.where(live > c, goal, -1)
        spread = spread + jnp.where(lane == order * capacity + c, goal, 0)
    target = jnp.sum(spread, axis=0, keepdims=True)
    row = lax.broadcasted_iota(jnp.int32, (rows_here, slots), 0)
    picker[...] = jnp.where(row == target, 1.0, 0.0).astype(jnp.bfloat16)

    loads[1].wait()
    loads[2].wait()
    own.wait()
    drain(landed.at[:, pl.ds(0, len(near))], near_recv)

    def step(g, total):
        cols = pl.ds(pl.multiple_of(g * LANES, LANES), LANES)
        block = landed[g].reshape(slots, LANES)
        gradient = jnp.dot(picker[...], block, preferred_element_type=jnp.float32)
        new_moment = beta_one * moment_out[:, cols] + (1.0 - beta_one) * gradient
        new_second = (
            beta_two * second_out[:, cols] + (1.0 - beta_two) * gradient * gradient
        )
        update = (
            new_moment / (jnp.sqrt(new_second) + epsilon)
            + decay * weight_out[:, cols]
        )
        moment_out[:, cols] = new_moment
        second_out[:, cols] = new_second
        update_out[:, cols] = update
        return total + jnp.sum(
            (update * update).reshape(rows_here // 8, 8, LANES), axis=0
        )

    update_sum = zero
    start = 0
    for q, size in enumerate(sizes):
        if far:
            drain(landed.at[pl.ds(start, size), pl.ds(0, len(far))], tile_recv.at[q])
        update_sum = lax.fori_loop(start, start + size, step, update_sum, unroll=min(size, 4))
        start += size

    update_row = jnp.sum(update_sum, axis=0, keepdims=True)
    update_row = update_row + pltpu.roll(update_row, LANES // 2, 1)
    left = lax.broadcasted_iota(jnp.int32, (1, LANES), 1) < LANES // 2
    parts[me] = jnp.where(left, update_row, weight_row)
    for where, _ in far + near:
        mesh_copy(parts.at[me], parts.at[me], part_send, part_recv, where).start()

    for k, ref in enumerate(small):
        if line_peers:
            drain(ref.at[column, pl.ds(0, Z - 1)], line_send.at[k])
        if plane_peers:
            drain(ref.at[pl.ds(0, columns - 1)], plane_send.at[k])
    drain(landed.at[:, pl.ds(0, len(near))], near_send)
    start = 0
    for q, size in enumerate(sizes):
        if far:
            drain(landed.at[pl.ds(start, size), pl.ds(0, len(far))], tile_send.at[q])
        start += size
    few = parts.at[pl.ds(0, n - 1)]
    drain(few, part_recv)
    total = jnp.sum(parts[...], axis=0)
    update_sq = jnp.sum(jnp.where(left, total, 0.0), axis=1, keepdims=True)
    weight_sq = jnp.sum(jnp.where(left, 0.0, total), axis=1, keepdims=True)
    trust = jnp.sqrt(weight_sq) / jnp.sqrt(update_sq + 1e-06)
    scale_out[...] = jnp.broadcast_to(rate * trust, scale_out.shape)
    drain(few, part_send)


def finish(
    weight, moment, second, update, scale,
    weight_out, moment_out, second_out, fresh, sem, piece_sem,
):
    copies = [
        pltpu.make_async_copy(moment, moment_out, sem.at[0]),
        pltpu.make_async_copy(second, second_out, sem.at[1]),
    ]
    for copy in copies:
        copy.start()
    rows_here = weight.shape[0]
    pieces = piece_sem.shape[0]
    height = rows_here // pieces
    factor = scale[0:1, 0:1]
    out = []
    for p in range(pieces):
        span = pl.ds(p * height, height)
        fresh[span, :] = weight[span, :] - factor * update[span, :]
        copy = pltpu.make_async_copy(
            fresh.at[span], weight_out.at[span], piece_sem.at[p]
        )
        copy.start()
        out.append(copy)
    for copy in copies + out:
        copy.wait()


def local(grid, weights, moment, second, tile_rows, row_index, bucket_count):
    Z, L, X, C = grid
    n = Z * L * X * C
    rows_here, width = weights.shape
    slots = row_index.shape[0]
    capacity = slots // n
    groups = width // LANES
    pack = 8 // capacity
    tiles = tile_rows.reshape(n // pack, pack, capacity, groups, LANES)
    tiles = tiles.transpose(0, 3, 1, 2, 4)
    table = (rows_here, width)
    anywhere = pl.BlockSpec(memory_space=pl.ANY)
    outside = pl.BlockSpec(memory_space=pltpu.HBM)
    inside = pl.BlockSpec(memory_space=pltpu.VMEM)
    f32 = jnp.float32
    dma = pltpu.SemaphoreType.DMA
    held = pltpu.VMEM(table, f32)
    chunks = len(pieces_of(groups))
    weight_v, moment_v, second_v, update_v, scale = pl.pallas_call(
        functools.partial(exchange, grid),
        out_shape=[jax.ShapeDtypeStruct(table, f32)] * 4
        + [jax.ShapeDtypeStruct((8, LANES), f32)],
        in_specs=[outside] * 6,
        out_specs=[inside] * 5,
        scratch_shapes=[
            pltpu.VMEM(tiles.shape, jnp.bfloat16),
            pltpu.VMEM((groups, n, capacity, LANES), jnp.bfloat16),
            pltpu.VMEM((L * X * C, Z, 1, slots), jnp.int32),
            pltpu.VMEM((L * X * C, Z, 1, n), jnp.int32),
            pltpu.VMEM((n, 1, LANES), f32),
            pltpu.VMEM((rows_here, slots), jnp.bfloat16),
            dma((3,)),
            dma((3,)),
            dma,
            pltpu.SemaphoreType.REGULAR,
            dma, dma,
            dma((chunks,)),
            dma((chunks,)),
            dma((2,)), dma((2,)), dma((2,)), dma((2,)), dma, dma,
        ],
        compiler_params=pltpu.CompilerParams(
            collective_id=0, has_side_effects=True, vmem_limit_bytes=24 * 1024 * 1024
        ),
        name="exchange",
    )(*(
        pltpu.with_memory_space_constraint(x, pltpu.HBM)
        for x in (
            weights, moment, second, tiles,
            row_index.reshape(1, slots), bucket_count.reshape(1, n),
        )
    ))
    pieces = 6
    return tuple(pl.pallas_call(
        finish,
        out_shape=[jax.ShapeDtypeStruct(table, f32)] * 3,
        in_specs=[inside] * 5,
        out_specs=[anywhere] * 3,
        scratch_shapes=[held, dma((2,)), dma((pieces,))],
        compiler_params=pltpu.CompilerParams(vmem_limit_bytes=24 * 1024 * 1024),
        name="finish",
    )(weight_v, moment_v, second_v, update_v, scale))


def solution(mesh):
    grid = factors(mesh.shape["rows"], mesh.shape["dp"])
    rows, flat = P(AXES, None), P(AXES)
    return jax.shard_map(
        functools.partial(local, grid),
        mesh=mesh,
        in_specs=(rows, rows, rows, rows, flat, flat),
        out_specs=(rows, rows, rows),
        check_vma=False,
    )
```

```python
import functools

import jax
import jax.numpy as jnp
from jax import lax
from jax.experimental import pallas as pl
from jax.experimental.pallas import tpu as pltpu
from jax.sharding import PartitionSpec as P

beta_one = 0.9
beta_two = 0.999
epsilon = 1e-06
decay = 0.01
rate = 0.1

AXES = ("rows", "dp")
LANES = 128


def factors(rows, dp):
    lo = max(d for d in range(1, rows + 1) if rows % d == 0 and d * d <= rows)
    core = 2 if dp % 2 == 0 else 1
    return rows // lo, lo, dp // core, core


def pieces_of(groups):
    big = max(groups // 8, 1)
    sizes = [big] * (groups // big)
    if big > 1:
        sizes[-1:] = [big - big // 2, big // 2]
    return sizes


def exchange(
    grid, weights, moment, second, tiles, index, count,
    weight_out, moment_out, second_out, update_out, sums_out,
    staged, landed, index_all, count_all, parts, picker, moment_in, second_in, decayed,
    load_sem, stage_sem, own_sem, ready, tile_send, near_recv, far_recv, chunk_recv,
    line_send, line_recv, plane_send, plane_recv, part_send, part_recv,
):
    Z, L, X, C = grid
    n = Z * L * X * C
    fast = X * C
    columns = L * X * C
    row_id, dp_id = lax.axis_index("rows"), lax.axis_index("dp")
    me = row_id * fast + dp_id
    hi, lo = row_id // L, lax.rem(row_id, L)
    x, core = dp_id // C, lax.rem(dp_id, C)
    column = lo * fast + dp_id
    rows_here, width = weights.shape
    groups = width // LANES
    slots = index.shape[-1]
    capacity = slots // n
    pack = tiles.shape[2]
    sizes = pieces_of(groups)

    half = Z // 2 if Z % 2 == 0 else 0
    if half:
        side = hi // half
        inside = hi - side * half
        line = [side * k + (1 - side) * (Z - 1 - k) for k in range(half)]
        line += [side * half + lax.rem(inside + j, half) for j in range(1, half)]
    else:
        line = [lax.rem(hi + j, Z) for j in range(1, Z)]
    los = [lo] + [lax.rem(lo + j, L) for j in range(1, L)]
    xs = [x] + [lax.rem(x + j, X) for j in range(1, X)]
    cores = [core] + [lax.rem(core + j, C) for j in range(1, C)]

    def spot(h, a, b, c):
        r, d = h * L + a, b * C + c
        return {"rows": r, "dp": d}, r * fast + d

    others = [
        (a, b, c)
        for j, a in list(enumerate(los))[::-1]
        for k, b in list(enumerate(xs))[::-1]
        if j or k
        for c in cores
    ]
    line_peers = [spot(h, lo, x, core) for h in line]
    plane_peers = [spot(hi, a, b, c) for a, b, c in others]
    plane_peers += [spot(hi, lo, x, c) for c in cores[1:]]
    near = [spot(h, lo, x, c) for h in line for c in cores] + plane_peers
    cross = [spot(h, a, b, c) for h in line[:half] for a, b, c in others]
    beside = [spot(h, a, b, c) for h in line[half:] for a, b, c in others]

    def mesh_copy(src, dst, send, recv, where):
        return pltpu.make_async_remote_copy(
            src_ref=src, dst_ref=dst, send_sem=send, recv_sem=recv,
            device_id=where, device_id_type=pl.DeviceIdType.MESH,
        )

    def drain(ref, sem):
        pltpu.make_async_copy(ref, ref, sem).wait()

    def send_rows(peers, start, size, recv):
        span = pl.ds(start, size)
        for where, peer in peers:
            mesh_copy(
                staged.at[peer // pack, span, lax.rem(peer, pack)],
                landed.at[span, me], tile_send, recv, where,
            ).start()

    stage = [
        pltpu.make_async_copy(tiles, staged, stage_sem.at[0]),
        pltpu.make_async_copy(index, index_all.at[column, hi], stage_sem.at[1]),
        pltpu.make_async_copy(count, count_all.at[column, hi], stage_sem.at[2]),
    ]
    for copy in stage:
        copy.start()
    barrier = pltpu.get_barrier_semaphore()
    for where, _ in near:
        pl.semaphore_signal(
            barrier, inc=1, device_id=where, device_id_type=pl.DeviceIdType.MESH
        )
    own = pltpu.make_async_copy(
        tiles.at[me // pack, :, lax.rem(me, pack)], landed.at[:, me], own_sem
    )
    own.start()
    loads = [
        pltpu.make_async_copy(weights, weight_out, load_sem.at[0]),
        pltpu.make_async_copy(moment, moment_in, load_sem.at[1]),
        pltpu.make_async_copy(second, second_in, load_sem.at[2]),
    ]
    for load in loads:
        load.start()
    for copy in stage:
        copy.wait()
    pl.semaphore_wait(barrier, len(near))

    for where, _ in line_peers:
        pl.semaphore_signal(
            ready, inc=1, device_id=where, device_id_type=pl.DeviceIdType.MESH
        )
    small = (index_all, count_all)
    for k, ref in enumerate(small):
        mine = ref.at[column, hi]
        for where, _ in line_peers:
            mesh_copy(mine, mine, line_send.at[k], line_recv.at[k], where).start()
    send_rows(near, 0, groups, near_recv)

    if line_peers:
        pl.semaphore_wait(ready, len(line_peers))
    end = (hi == 0) | (hi == Z - 1)
    inner = jnp.logical_not(end)
    aside = len(others)

    def send_chunks(peers, some):
        for q in some:
            send_rows(peers, sum(sizes[:q]), sizes[q], chunk_recv.at[q])

    chunks = range(len(sizes))
    soon = len(sizes) // 2

    if half:
        pl.when(end)(lambda: send_rows(cross, 0, groups, far_recv))
        if half > 1:
            @pl.when(inner)
            def _():
                send_chunks(cross, chunks[:soon])
                send_rows(beside, 0, groups, far_recv)

    else:
        send_rows(beside, 0, groups, far_recv)
    for k, ref in enumerate(small):
        if line_peers:
            drain(ref.at[column, pl.ds(0, Z - 1)], line_recv.at[k])
        block = ref.at[column]
        for where, _ in plane_peers:
            mesh_copy(block, block, plane_send.at[k], plane_recv.at[k], where).start()
    if half > 1:
        pl.when(end)(lambda: send_chunks(beside, chunks))
        pl.when(inner)(lambda: send_chunks(cross, chunks[soon:]))

    loads[0].wait()

    def columns_of(g):
        return pl.ds(pl.multiple_of(g * LANES, LANES), LANES)

    def weight_step(g, total):
        w = weight_out[:, columns_of(g)]
        decayed[:, columns_of(g)] = decay * w
        return total + jnp.sum((w * w).reshape(rows_here // 8, 8, LANES), axis=0)

    zero = jnp.zeros((8, LANES), jnp.float32)
    weight_sum = lax.fori_loop(0, groups, weight_step, zero, unroll=4)
    weight_row = jnp.sum(weight_sum, axis=0, keepdims=True)
    weight_row = weight_row + pltpu.roll(weight_row, LANES // 2, 1)

    loads[1].wait()
    loads[2].wait()

    @pl.loop(0, groups, unroll=4)
    def _(g):
        moment_in[:, columns_of(g)] = beta_one * moment_in[:, columns_of(g)]
        second_in[:, columns_of(g)] = beta_two * second_in[:, columns_of(g)]

    if plane_peers:
        for k, ref in enumerate(small):
            drain(ref.at[pl.ds(0, columns - 1)], plane_recv.at[k])
    index_rows = jnp.concatenate([index_all[:, h, 0, :] for h in range(Z)], axis=0)
    count_rows = jnp.concatenate([count_all[:, h, 0, :] for h in range(Z)], axis=0)
    lane = lax.broadcasted_iota(jnp.int32, (n, slots), 1)
    order = lax.broadcasted_iota(jnp.int32, (n, slots), 0)
    owner = lax.broadcasted_iota(jnp.int32, (n, n), 1)
    live = jnp.sum(jnp.where(owner == me, count_rows, 0), axis=1, keepdims=True)
    spread = jnp.zeros((n, slots), jnp.int32)
    for c in range(capacity):
        goal = jnp.sum(
            jnp.where(lane == me * capacity + c, index_rows, 0), axis=1, keepdims=True
        )
        goal = jnp.where(live > c, goal, -1)
        spread = spread + jnp.where(lane == order * capacity + c, goal, 0)
    target = jnp.sum(spread, axis=0, keepdims=True)
    row = lax.broadcasted_iota(jnp.int32, (rows_here, slots), 0)
    picker[...] = jnp.where(row == target, 1.0, 0.0).astype(jnp.bfloat16)

    own.wait()
    drain(landed.at[:, pl.ds(0, len(near))], near_recv)

    def arrived(start, size, from_end, from_inner, sem):
        def take(planes):
            if planes * aside:
                drain(landed.at[pl.ds(start, size), pl.ds(0, planes * aside)], sem)

        if half > 1:
            pl.when(end)(lambda: take(from_end))
            pl.when(inner)(lambda: take(from_inner))
        else:
            take(from_end)

    arrived(0, groups, half if half else Z - 1, half - 1, far_recv)

    def step(g, total):
        cols = columns_of(g)
        block = landed[g].reshape(slots, LANES)
        gradient = jnp.dot(picker[...], block, preferred_element_type=jnp.float32)
        new_moment = moment_in[:, cols] + (1.0 - beta_one) * gradient
        new_second = second_in[:, cols] + (1.0 - beta_two) * gradient * gradient
        root = new_second * lax.rsqrt(new_second)
        update = new_moment / (root + epsilon) + decayed[:, cols]
        moment_out[:, cols] = new_moment
        second_out[:, cols] = new_second
        update_out[:, cols] = update
        return total + jnp.sum(
            (update * update).reshape(rows_here // 8, 8, LANES), axis=0
        )

    update_sum = zero
    start = 0
    for q, size in enumerate(sizes):
        arrived(start, size, half - 1 if half else 0, half, chunk_recv.at[q])
        update_sum = lax.fori_loop(
            start, start + size, step, update_sum, unroll=min(size, 4)
        )
        start += size

    update_row = jnp.sum(update_sum, axis=0, keepdims=True)
    update_row = update_row + pltpu.roll(update_row, LANES // 2, 1)
    left = lax.broadcasted_iota(jnp.int32, (1, LANES), 1) < LANES // 2
    parts[me] = jnp.where(left, update_row, weight_row)
    for where, _ in cross + beside + near:
        mesh_copy(parts.at[me], parts.at[me], part_send, part_recv, where).start()

    for k, ref in enumerate(small):
        if line_peers:
            drain(ref.at[column, pl.ds(0, Z - 1)], line_send.at[k])
        if plane_peers:
            drain(ref.at[pl.ds(0, columns - 1)], plane_send.at[k])
    drain(landed.at[:, pl.ds(0, n - 1)], tile_send)
    few = parts.at[pl.ds(0, n - 1)]
    drain(few, part_recv)
    sums_out[...] = jnp.sum(parts[...], axis=0)
    drain(few, part_send)


def finish(
    weight, moment, second, update, sums,
    weight_out, moment_out, second_out, fresh, sem, piece_sem,
):
    copies = [
        pltpu.make_async_copy(moment, moment_out, sem.at[0]),
        pltpu.make_async_copy(second, second_out, sem.at[1]),
    ]
    for copy in copies:
        copy.start()
    rows_here = weight.shape[0]
    pieces = piece_sem.shape[0]
    height = rows_here // pieces
    total = sums[...]
    left = lax.broadcasted_iota(jnp.int32, total.shape, 1) < LANES // 2
    update_sq = jnp.sum(jnp.where(left, total, 0.0), axis=1, keepdims=True)
    weight_sq = jnp.sum(jnp.where(left, 0.0, total), axis=1, keepdims=True)
    trust = jnp.sqrt(weight_sq) / jnp.sqrt(update_sq + 1e-06)
    factor = rate * trust
    out = []
    for p in range(pieces):
        span = pl.ds(p * height, height)
        fresh[span, :] = weight[span, :] - factor * update[span, :]
        copy = pltpu.make_async_copy(
            fresh.at[span], weight_out.at[span], piece_sem.at[p]
        )
        copy.start()
        out.append(copy)
    for copy in copies + out:
        copy.wait()


def local(grid, weights, moment, second, tile_rows, row_index, bucket_count):
    Z, L, X, C = grid
    n = Z * L * X * C
    rows_here, width = weights.shape
    slots = row_index.shape[0]
    capacity = slots // n
    groups = width // LANES
    pack = 8 // capacity
    tiles = tile_rows.reshape(n // pack, pack, capacity, groups, LANES)
    tiles = tiles.transpose(0, 3, 1, 2, 4)
    table = (rows_here, width)
    anywhere = pl.BlockSpec(memory_space=pl.ANY)
    outside = pl.BlockSpec(memory_space=pltpu.HBM)
    inside = pl.BlockSpec(memory_space=pltpu.VMEM)
    f32 = jnp.float32
    dma = pltpu.SemaphoreType.DMA
    held = pltpu.VMEM(table, f32)
    weight_v, moment_v, second_v, update_v, sums = pl.pallas_call(
        functools.partial(exchange, grid),
        out_shape=[jax.ShapeDtypeStruct(table, f32)] * 4
        + [jax.ShapeDtypeStruct((1, LANES), f32)],
        in_specs=[outside] * 6,
        out_specs=[inside] * 5,
        scratch_shapes=[
            pltpu.VMEM(tiles.shape, jnp.bfloat16),
            pltpu.VMEM((groups, n, capacity, LANES), jnp.bfloat16),
            pltpu.VMEM((L * X * C, Z, 1, slots), jnp.int32),
            pltpu.VMEM((L * X * C, Z, 1, n), jnp.int32),
            pltpu.VMEM((n, 1, LANES), f32),
            pltpu.VMEM((rows_here, slots), jnp.bfloat16),
            held, held, held,
            dma((3,)), dma((3,)), dma, pltpu.SemaphoreType.REGULAR,
            dma, dma, dma, dma((len(pieces_of(groups)),)),
            dma((2,)), dma((2,)), dma((2,)), dma((2,)), dma, dma,
        ],
        compiler_params=pltpu.CompilerParams(
            collective_id=0, has_side_effects=True, vmem_limit_bytes=36 * 1024 * 1024
        ),
        name="exchange",
    )(*(
        pltpu.with_memory_space_constraint(x, pltpu.HBM)
        for x in (
            weights, moment, second, tiles,
            row_index.reshape(1, slots), bucket_count.reshape(1, n),
        )
    ))
    pieces = 6
    return tuple(pl.pallas_call(
        finish,
        out_shape=[jax.ShapeDtypeStruct(table, f32)] * 3,
        in_specs=[inside] * 5,
        out_specs=[anywhere] * 3,
        scratch_shapes=[held, dma((2,)), dma((pieces,))],
        compiler_params=pltpu.CompilerParams(vmem_limit_bytes=24 * 1024 * 1024),
        name="finish",
    )(weight_v, moment_v, second_v, update_v, sums))


def solution(mesh):
    grid = factors(mesh.shape["rows"], mesh.shape["dp"])
    rows, flat = P(AXES, None), P(AXES)
    return jax.shard_map(
        functools.partial(local, grid),
        mesh=mesh,
        in_specs=(rows, rows, rows, rows, flat, flat),
        out_specs=(rows, rows, rows),
        check_vma=False,
    )
```

```python
import functools

import jax
import jax.numpy as jnp
from jax import lax
from jax.experimental import pallas as pl
from jax.experimental.pallas import tpu as pltpu
from jax.sharding import PartitionSpec as P

beta_one = 0.9
beta_two = 0.999
epsilon = 1e-06
decay = 0.01
rate = 0.1

AXES = ("rows", "dp")
LANES = 128


def factors(rows, dp):
    lo = max(d for d in range(1, rows + 1) if rows % d == 0 and d * d <= rows)
    core = 2 if dp % 2 == 0 else 1
    return rows // lo, lo, dp // core, core


def pieces_of(groups):
    big = groups * 3 // 8
    sizes = [big, big, groups - 2 * big] if big else [groups]
    return sizes


def exchange(
    grid, weights, moment, second, tiles, index, count,
    weight_out, moment_out, second_out, update_out, sums_out,
    staged, landed, index_all, count_all, parts, picker, moment_in, second_in, decayed,
    load_sem, stage_sem, own_sem, ready, tile_send, near_recv, far_recv, chunk_recv,
    line_send, line_recv, plane_send, plane_recv, part_send, part_recv,
):
    Z, L, X, C = grid
    n = Z * L * X * C
    fast = X * C
    columns = L * X * C
    row_id, dp_id = lax.axis_index("rows"), lax.axis_index("dp")
    me = row_id * fast + dp_id
    hi, lo = row_id // L, lax.rem(row_id, L)
    x, core = dp_id // C, lax.rem(dp_id, C)
    column = lo * fast + dp_id
    rows_here, width = weights.shape
    groups = width // LANES
    slots = index.shape[-1]
    capacity = slots // n
    pack = tiles.shape[2]
    sizes = pieces_of(groups)

    half = Z // 2 if Z % 2 == 0 else 0
    if half:
        side = hi // half
        inside = hi - side * half
        line = [side * k + (1 - side) * (Z - 1 - k) for k in range(half)]
        line += [side * half + lax.rem(inside + j, half) for j in range(1, half)]
    else:
        line = [lax.rem(hi + j, Z) for j in range(1, Z)]
    los = [lo] + [lax.rem(lo + j, L) for j in range(1, L)]
    xs = [x] + [lax.rem(x + j, X) for j in range(1, X)]
    cores = [core] + [lax.rem(core + j, C) for j in range(1, C)]

    def spot(h, a, b, c):
        r, d = h * L + a, b * C + c
        return {"rows": r, "dp": d}, r * fast + d

    others = [
        (a, b, c)
        for j, a in list(enumerate(los))[::-1]
        for k, b in list(enumerate(xs))[::-1]
        if j or k
        for c in cores
    ]
    line_peers = [spot(h, lo, x, core) for h in line]
    plane_peers = [spot(hi, a, b, c) for a, b, c in others]
    plane_peers += [spot(hi, lo, x, c) for c in cores[1:]]
    near = [spot(h, lo, x, c) for h in line for c in cores] + plane_peers
    cross = [spot(h, a, b, c) for h in line[:half] for a, b, c in others]
    beside = [spot(h, a, b, c) for h in line[half:] for a, b, c in others]

    def mesh_copy(src, dst, send, recv, where):
        return pltpu.make_async_remote_copy(
            src_ref=src, dst_ref=dst, send_sem=send, recv_sem=recv,
            device_id=where, device_id_type=pl.DeviceIdType.MESH,
        )

    def drain(ref, sem):
        pltpu.make_async_copy(ref, ref, sem).wait()

    def send_rows(peers, start, size, recv):
        span = pl.ds(start, size)
        for where, peer in peers:
            mesh_copy(
                staged.at[peer // pack, span, lax.rem(peer, pack)],
                landed.at[span, me], tile_send, recv, where,
            ).start()

    stage = [
        pltpu.make_async_copy(tiles, staged, stage_sem.at[0]),
        pltpu.make_async_copy(index, index_all.at[column, hi], stage_sem.at[1]),
        pltpu.make_async_copy(count, count_all.at[column, hi], stage_sem.at[2]),
    ]
    for copy in stage:
        copy.start()
    barrier = pltpu.get_barrier_semaphore()
    for where, _ in near:
        pl.semaphore_signal(
            barrier, inc=1, device_id=where, device_id_type=pl.DeviceIdType.MESH
        )
    own = pltpu.make_async_copy(
        tiles.at[me // pack, :, lax.rem(me, pack)], landed.at[:, me], own_sem
    )
    own.start()
    loads = [
        pltpu.make_async_copy(weights, weight_out, load_sem.at[0]),
        pltpu.make_async_copy(moment, moment_in, load_sem.at[1]),
        pltpu.make_async_copy(second, second_in, load_sem.at[2]),
    ]
    for copy in stage:
        copy.wait()
    for load in loads:
        load.start()
    pl.semaphore_wait(barrier, len(near))

    for where, _ in line_peers:
        pl.semaphore_signal(
            ready, inc=1, device_id=where, device_id_type=pl.DeviceIdType.MESH
        )
    small = (index_all, count_all)
    for k, ref in enumerate(small):
        mine = ref.at[column, hi]
        for where, _ in line_peers:
            mesh_copy(mine, mine, line_send.at[k], line_recv.at[k], where).start()
    send_rows(near, 0, groups, near_recv)

    if line_peers:
        pl.semaphore_wait(ready, len(line_peers))
    end = (hi == 0) | (hi == Z - 1)
    inner = jnp.logical_not(end)
    aside = len(others)

    def send_chunks(peers):
        for q, size in enumerate(sizes):
            send_rows(peers, sum(sizes[:q]), size, chunk_recv.at[q])

    if half:
        pl.when(end)(lambda: send_rows(cross, 0, groups, far_recv))
        if half > 1:
            pl.when(inner)(lambda: send_rows(beside + cross[:aside], 0, groups, far_recv))

    else:
        send_rows(beside, 0, groups, far_recv)
    for k, ref in enumerate(small):
        if line_peers:
            drain(ref.at[column, pl.ds(0, Z - 1)], line_recv.at[k])
        block = ref.at[column]
        for where, _ in plane_peers:
            mesh_copy(block, block, plane_send.at[k], plane_recv.at[k], where).start()
    if half > 1:
        pl.when(end)(lambda: send_chunks(beside))
        pl.when(inner)(lambda: send_chunks(cross[aside:]))

    loads[0].wait()

    def columns_of(g):
        return pl.ds(pl.multiple_of(g * LANES, LANES), LANES)

    def weight_step(g, total):
        w = weight_out[:, columns_of(g)]
        decayed[:, columns_of(g)] = decay * w
        return total + jnp.sum((w * w).reshape(rows_here // 8, 8, LANES), axis=0)

    zero = jnp.zeros((8, LANES), jnp.float32)
    weight_sum = lax.fori_loop(0, groups, weight_step, zero, unroll=4)
    weight_row = jnp.sum(weight_sum, axis=0, keepdims=True)
    weight_row = weight_row + pltpu.roll(weight_row, LANES // 2, 1)

    loads[1].wait()
    loads[2].wait()

    @pl.loop(0, groups, unroll=4)
    def _(g):
        moment_in[:, columns_of(g)] = beta_one * moment_in[:, columns_of(g)]
        second_in[:, columns_of(g)] = beta_two * second_in[:, columns_of(g)]

    if plane_peers:
        for k, ref in enumerate(small):
            drain(ref.at[pl.ds(0, columns - 1)], plane_recv.at[k])
    index_rows = jnp.concatenate([index_all[:, h, 0, :] for h in range(Z)], axis=0)
    count_rows = jnp.concatenate([count_all[:, h, 0, :] for h in range(Z)], axis=0)
    lane = lax.broadcasted_iota(jnp.int32, (n, slots), 1)
    order = lax.broadcasted_iota(jnp.int32, (n, slots), 0)
    owner = lax.broadcasted_iota(jnp.int32, (n, n), 1)
    live = jnp.sum(jnp.where(owner == me, count_rows, 0), axis=1, keepdims=True)
    spread = jnp.zeros((n, slots), jnp.int32)
    for c in range(capacity):
        goal = jnp.sum(
            jnp.where(lane == me * capacity + c, index_rows, 0), axis=1, keepdims=True
        )
        goal = jnp.where(live > c, goal, -1)
        spread = spread + jnp.where(lane == order * capacity + c, goal, 0)
    target = jnp.sum(spread, axis=0, keepdims=True)
    row = lax.broadcasted_iota(jnp.int32, (rows_here, slots), 0)
    picker[...] = jnp.where(row == target, 1.0, 0.0).astype(jnp.bfloat16)

    own.wait()
    drain(landed.at[:, pl.ds(0, len(near))], near_recv)

    def arrived(start, size, from_end, from_inner, sem):
        def take(planes):
            if planes * aside:
                drain(landed.at[pl.ds(start, size), pl.ds(0, planes * aside)], sem)

        if half > 1:
            pl.when(end)(lambda: take(from_end))
            pl.when(inner)(lambda: take(from_inner))
        else:
            take(from_end)

    arrived(0, groups, 2 * half - 1 if half else Z - 1, half - 1, far_recv)

    def step(g, total):
        cols = columns_of(g)
        block = landed[g].reshape(slots, LANES)
        gradient = jnp.dot(picker[...], block, preferred_element_type=jnp.float32)
        new_moment = moment_in[:, cols] + (1.0 - beta_one) * gradient
        new_second = second_in[:, cols] + (1.0 - beta_two) * gradient * gradient
        root = new_second * lax.rsqrt(new_second)
        update = new_moment / (root + epsilon) + decayed[:, cols]
        moment_out[:, cols] = new_moment
        second_out[:, cols] = new_second
        update_out[:, cols] = update
        return total + jnp.sum(
            (update * update).reshape(rows_here // 8, 8, LANES), axis=0
        )

    update_sum = zero
    start = 0
    for q, size in enumerate(sizes):
        arrived(start, size, 0, half, chunk_recv.at[q])
        update_sum = lax.fori_loop(
            start, start + size, step, update_sum, unroll=size
        )
        start += size

    update_row = jnp.sum(update_sum, axis=0, keepdims=True)
    update_row = update_row + pltpu.roll(update_row, LANES // 2, 1)
    left = lax.broadcasted_iota(jnp.int32, (1, LANES), 1) < LANES // 2
    parts[me] = jnp.where(left, update_row, weight_row)
    for where, _ in cross + beside + near:
        mesh_copy(parts.at[me], parts.at[me], part_send, part_recv, where).start()

    for k, ref in enumerate(small):
        if line_peers:
            drain(ref.at[column, pl.ds(0, Z - 1)], line_send.at[k])
        if plane_peers:
            drain(ref.at[pl.ds(0, columns - 1)], plane_send.at[k])
    drain(landed.at[:, pl.ds(0, n - 1)], tile_send)
    few = parts.at[pl.ds(0, n - 1)]
    drain(few, part_recv)
    sums_out[...] = jnp.sum(parts[...], axis=0)
    drain(few, part_send)


def finish(
    weight, moment, second, update, sums,
    weight_out, moment_out, second_out, fresh, sem, piece_sem,
):
    copies = [
        pltpu.make_async_copy(moment, moment_out, sem.at[0]),
        pltpu.make_async_copy(second, second_out, sem.at[1]),
    ]
    for copy in copies:
        copy.start()
    rows_here = weight.shape[0]
    pieces = piece_sem.shape[0]
    height = rows_here // pieces
    total = sums[...]
    left = lax.broadcasted_iota(jnp.int32, total.shape, 1) < LANES // 2
    update_sq = jnp.sum(jnp.where(left, total, 0.0), axis=1, keepdims=True)
    weight_sq = jnp.sum(jnp.where(left, 0.0, total), axis=1, keepdims=True)
    trust = jnp.sqrt(weight_sq) / jnp.sqrt(update_sq + 1e-06)
    factor = rate * trust
    out = []
    for p in range(pieces):
        span = pl.ds(p * height, height)
        fresh[span, :] = weight[span, :] - factor * update[span, :]
        copy = pltpu.make_async_copy(
            fresh.at[span], weight_out.at[span], piece_sem.at[p]
        )
        copy.start()
        out.append(copy)
    for copy in copies + out:
        copy.wait()


def local(grid, weights, moment, second, tile_rows, row_index, bucket_count):
    Z, L, X, C = grid
    n = Z * L * X * C
    rows_here, width = weights.shape
    slots = row_index.shape[0]
    capacity = slots // n
    groups = width // LANES
    pack = 8 // capacity
    tiles = tile_rows.reshape(n // pack, pack, capacity, groups, LANES)
    tiles = tiles.transpose(0, 3, 1, 2, 4)
    table = (rows_here, width)
    anywhere = pl.BlockSpec(memory_space=pl.ANY)
    outside = pl.BlockSpec(memory_space=pltpu.HBM)
    inside = pl.BlockSpec(memory_space=pltpu.VMEM)
    f32 = jnp.float32
    dma = pltpu.SemaphoreType.DMA
    held = pltpu.VMEM(table, f32)
    weight_v, moment_v, second_v, update_v, sums = pl.pallas_call(
        functools.partial(exchange, grid),
        out_shape=[jax.ShapeDtypeStruct(table, f32)] * 4
        + [jax.ShapeDtypeStruct((1, LANES), f32)],
        in_specs=[outside] * 6,
        out_specs=[inside] * 5,
        scratch_shapes=[
            pltpu.VMEM(tiles.shape, jnp.bfloat16),
            pltpu.VMEM((groups, n, capacity, LANES), jnp.bfloat16),
            pltpu.VMEM((L * X * C, Z, 1, slots), jnp.int32),
            pltpu.VMEM((L * X * C, Z, 1, n), jnp.int32),
            pltpu.VMEM((n, 1, LANES), f32),
            pltpu.VMEM((rows_here, slots), jnp.bfloat16),
            held, held, held,
            dma((3,)), dma((3,)), dma, pltpu.SemaphoreType.REGULAR,
            dma, dma, dma, dma((len(pieces_of(groups)),)),
            dma((2,)), dma((2,)), dma((2,)), dma((2,)), dma, dma,
        ],
        compiler_params=pltpu.CompilerParams(
            collective_id=0, has_side_effects=True, vmem_limit_bytes=36 * 1024 * 1024
        ),
        name="exchange",
    )(*(
        pltpu.with_memory_space_constraint(x, pltpu.HBM)
        for x in (
            weights, moment, second, tiles,
            row_index.reshape(1, slots), bucket_count.reshape(1, n),
        )
    ))
    pieces = 6
    return tuple(pl.pallas_call(
        finish,
        out_shape=[jax.ShapeDtypeStruct(table, f32)] * 3,
        in_specs=[inside] * 5,
        out_specs=[anywhere] * 3,
        scratch_shapes=[held, dma((2,)), dma((pieces,))],
        compiler_params=pltpu.CompilerParams(vmem_limit_bytes=24 * 1024 * 1024),
        name="finish",
    )(weight_v, moment_v, second_v, update_v, sums))


def solution(mesh):
    grid = factors(mesh.shape["rows"], mesh.shape["dp"])
    rows, flat = P(AXES, None), P(AXES)
    return jax.shard_map(
        functools.partial(local, grid),
        mesh=mesh,
        in_specs=(rows, rows, rows, rows, flat, flat),
        out_specs=(rows, rows, rows),
        check_vma=False,
    )
```

```python
import functools

import jax
import jax.numpy as jnp
from jax import lax
from jax.experimental import pallas as pl
from jax.experimental.pallas import tpu as pltpu
from jax.sharding import PartitionSpec as P

beta_one = 0.9
beta_two = 0.999
epsilon = 1e-06
decay = 0.01
rate = 0.1

AXES = ("rows", "dp")
LANES = 128


def factors(rows, dp):
    lo = max(d for d in range(1, rows + 1) if rows % d == 0 and d * d <= rows)
    core = 2 if dp % 2 == 0 else 1
    return rows // lo, lo, dp // core, core


def pieces_of(groups):
    small = groups // 4
    half = (groups - small) // 2
    sizes = [size for size in (small, half, groups - small - half) if size]
    return sizes


def exchange(
    grid, weights, moment, second, tiles, index, count,
    weight_out, moment_out, second_out, update_out, sums_out,
    staged, landed, index_all, count_all, parts, picker, moment_in, second_in, decayed,
    load_sem, stage_sem, own_sem, ready, tile_send, near_recv, far_recv, chunk_recv,
    line_send, line_recv, plane_send, plane_recv, part_send, part_recv,
):
    Z, L, X, C = grid
    n = Z * L * X * C
    fast = X * C
    columns = L * X * C
    row_id, dp_id = lax.axis_index("rows"), lax.axis_index("dp")
    me = row_id * fast + dp_id
    hi, lo = row_id // L, lax.rem(row_id, L)
    x, core = dp_id // C, lax.rem(dp_id, C)
    column = lo * fast + dp_id
    rows_here, width = weights.shape
    groups = width // LANES
    slots = index.shape[-1]
    capacity = slots // n
    pack = tiles.shape[2]
    sizes = pieces_of(groups)

    half = Z // 2 if Z % 2 == 0 else 0
    if half:
        side = hi // half
        inside = hi - side * half
        line = [side * k + (1 - side) * (Z - 1 - k) for k in range(half)]
        line += [side * half + lax.rem(inside + j, half) for j in range(1, half)]
    else:
        line = [lax.rem(hi + j, Z) for j in range(1, Z)]
    los = [lo] + [lax.rem(lo + j, L) for j in range(1, L)]
    xs = [x] + [lax.rem(x + j, X) for j in range(1, X)]
    cores = [core] + [lax.rem(core + j, C) for j in range(1, C)]

    def spot(h, a, b, c):
        r, d = h * L + a, b * C + c
        return {"rows": r, "dp": d}, r * fast + d

    others = [
        (a, b, c)
        for c in cores
        for j, a in list(enumerate(los))[::-1]
        for k, b in list(enumerate(xs))[::-1]
        if j or k
    ]
    line_peers = [spot(h, lo, x, core) for h in line]
    plane_peers = [spot(hi, a, b, c) for a, b, c in others]
    plane_peers += [spot(hi, lo, x, c) for c in cores[1:]]
    near = [spot(h, lo, x, c) for h in line for c in cores] + plane_peers
    cross = [spot(h, a, b, c) for h in line[:half] for a, b, c in others]
    beside = [spot(h, a, b, c) for h in line[half:] for a, b, c in others]

    def mesh_copy(src, dst, send, recv, where):
        return pltpu.make_async_remote_copy(
            src_ref=src, dst_ref=dst, send_sem=send, recv_sem=recv,
            device_id=where, device_id_type=pl.DeviceIdType.MESH,
        )

    def drain(ref, sem):
        pltpu.make_async_copy(ref, ref, sem).wait()

    def send_rows(peers, start, size, recv):
        span = pl.ds(start, size)
        for where, peer in peers:
            mesh_copy(
                staged.at[peer // pack, span, lax.rem(peer, pack)],
                landed.at[span, me], tile_send, recv, where,
            ).start()

    stage = [
        pltpu.make_async_copy(tiles, staged, stage_sem.at[0]),
        pltpu.make_async_copy(index, index_all.at[column, hi], stage_sem.at[1]),
        pltpu.make_async_copy(count, count_all.at[column, hi], stage_sem.at[2]),
    ]
    for copy in stage:
        copy.start()
    barrier = pltpu.get_barrier_semaphore()
    for where, _ in near:
        pl.semaphore_signal(
            barrier, inc=1, device_id=where, device_id_type=pl.DeviceIdType.MESH
        )
    own = pltpu.make_async_copy(
        tiles.at[me // pack, :, lax.rem(me, pack)], landed.at[:, me], own_sem
    )
    own.start()
    loads = [
        pltpu.make_async_copy(weights, weight_out, load_sem.at[0]),
        pltpu.make_async_copy(moment, moment_in, load_sem.at[1]),
        pltpu.make_async_copy(second, second_in, load_sem.at[2]),
    ]
    for copy in stage:
        copy.wait()
    for load in loads:
        load.start()
    pl.semaphore_wait(barrier, len(near))

    for where, _ in line_peers:
        pl.semaphore_signal(
            ready, inc=1, device_id=where, device_id_type=pl.DeviceIdType.MESH
        )
    small = (index_all, count_all)
    for k, ref in enumerate(small):
        mine = ref.at[column, hi]
        for where, _ in line_peers:
            mesh_copy(mine, mine, line_send.at[k], line_recv.at[k], where).start()
    send_rows(near, 0, groups, near_recv)

    if line_peers:
        pl.semaphore_wait(ready, len(line_peers))
    end = (hi == 0) | (hi == Z - 1)
    inner = jnp.logical_not(end)
    aside = len(others)

    def send_chunks(peers):
        for q, size in enumerate(sizes):
            send_rows(peers, sum(sizes[:q]), size, chunk_recv.at[q])

    if half:
        pl.when(end)(lambda: send_rows(cross, 0, groups, far_recv))
        if half > 1:
            pl.when(inner)(lambda: send_rows(beside + cross[:aside], 0, groups, far_recv))

    else:
        send_rows(beside, 0, groups, far_recv)
    for k, ref in enumerate(small):
        if line_peers:
            drain(ref.at[column, pl.ds(0, Z - 1)], line_recv.at[k])
        block = ref.at[column]
        for where, _ in plane_peers:
            mesh_copy(block, block, plane_send.at[k], plane_recv.at[k], where).start()
    if half > 1:
        pl.when(end)(lambda: send_chunks(beside))
        pl.when(inner)(lambda: send_chunks(cross[aside:]))

    loads[0].wait()

    def columns_of(g):
        return pl.ds(pl.multiple_of(g * LANES, LANES), LANES)

    def weight_step(g, total):
        w = weight_out[:, columns_of(g)]
        decayed[:, columns_of(g)] = decay * w
        return total + jnp.sum((w * w).reshape(rows_here // 8, 8, LANES), axis=0)

    zero = jnp.zeros((8, LANES), jnp.float32)
    weight_sum = lax.fori_loop(0, groups, weight_step, zero, unroll=4)
    weight_row = jnp.sum(weight_sum, axis=0, keepdims=True)
    weight_row = weight_row + pltpu.roll(weight_row, LANES // 2, 1)

    loads[1].wait()
    loads[2].wait()

    @pl.loop(0, groups, unroll=4)
    def _(g):
        moment_in[:, columns_of(g)] = beta_one * moment_in[:, columns_of(g)]
        second_in[:, columns_of(g)] = beta_two * second_in[:, columns_of(g)]

    if plane_peers:
        for k, ref in enumerate(small):
            drain(ref.at[pl.ds(0, columns - 1)], plane_recv.at[k])
    index_rows = jnp.concatenate([index_all[:, h, 0, :] for h in range(Z)], axis=0)
    count_rows = jnp.concatenate([count_all[:, h, 0, :] for h in range(Z)], axis=0)
    lane = lax.broadcasted_iota(jnp.int32, (n, slots), 1)
    order = lax.broadcasted_iota(jnp.int32, (n, slots), 0)
    owner = lax.broadcasted_iota(jnp.int32, (n, n), 1)
    live = jnp.sum(jnp.where(owner == me, count_rows, 0), axis=1, keepdims=True)
    spread = jnp.zeros((n, slots), jnp.int32)
    for c in range(capacity):
        goal = jnp.sum(
            jnp.where(lane == me * capacity + c, index_rows, 0), axis=1, keepdims=True
        )
        goal = jnp.where(live > c, goal, -1)
        spread = spread + jnp.where(lane == order * capacity + c, goal, 0)
    target = jnp.sum(spread, axis=0, keepdims=True)
    row = lax.broadcasted_iota(jnp.int32, (rows_here, slots), 0)
    picker[...] = jnp.where(row == target, 1.0, 0.0).astype(jnp.bfloat16)

    own.wait()
    drain(landed.at[:, pl.ds(0, len(near))], near_recv)

    def arrived(start, size, from_end, from_inner, sem):
        def take(planes):
            if planes * aside:
                drain(landed.at[pl.ds(start, size), pl.ds(0, planes * aside)], sem)

        if half > 1:
            pl.when(end)(lambda: take(from_end))
            pl.when(inner)(lambda: take(from_inner))
        else:
            take(from_end)

    arrived(0, groups, 2 * half - 1 if half else Z - 1, half - 1, far_recv)

    def step(g, total):
        cols = columns_of(g)
        block = landed[g].reshape(slots, LANES)
        gradient = jnp.dot(picker[...], block, preferred_element_type=jnp.float32)
        new_moment = moment_in[:, cols] + (1.0 - beta_one) * gradient
        new_second = second_in[:, cols] + (1.0 - beta_two) * gradient * gradient
        root = new_second * lax.rsqrt(new_second)
        update = new_moment / (root + epsilon) + decayed[:, cols]
        moment_out[:, cols] = new_moment
        second_out[:, cols] = new_second
        update_out[:, cols] = update
        return total + jnp.sum(
            (update * update).reshape(rows_here // 8, 8, LANES), axis=0
        )

    update_sum = zero
    start = 0
    for q, size in enumerate(sizes):
        arrived(start, size, 0, half, chunk_recv.at[q])
        update_sum = lax.fori_loop(
            start, start + size, step, update_sum, unroll=size
        )
        start += size

    update_row = jnp.sum(update_sum, axis=0, keepdims=True)
    update_row = update_row + pltpu.roll(update_row, LANES // 2, 1)
    left = lax.broadcasted_iota(jnp.int32, (1, LANES), 1) < LANES // 2
    parts[me] = jnp.where(left, update_row, weight_row)
    for where, _ in cross + beside + near:
        mesh_copy(parts.at[me], parts.at[me], part_send, part_recv, where).start()

    for k, ref in enumerate(small):
        if line_peers:
            drain(ref.at[column, pl.ds(0, Z - 1)], line_send.at[k])
        if plane_peers:
            drain(ref.at[pl.ds(0, columns - 1)], plane_send.at[k])
    drain(landed.at[:, pl.ds(0, n - 1)], tile_send)
    few = parts.at[pl.ds(0, n - 1)]
    drain(few, part_recv)
    sums_out[...] = jnp.sum(parts[...], axis=0)
    drain(few, part_send)


def finish(
    weight, moment, second, update, sums,
    weight_out, moment_out, second_out, fresh, sem, piece_sem,
):
    copies = [
        pltpu.make_async_copy(moment, moment_out, sem.at[0]),
        pltpu.make_async_copy(second, second_out, sem.at[1]),
    ]
    for copy in copies:
        copy.start()
    rows_here = weight.shape[0]
    pieces = piece_sem.shape[0]
    height = rows_here // pieces
    total = sums[...]
    left = lax.broadcasted_iota(jnp.int32, total.shape, 1) < LANES // 2
    update_sq = jnp.sum(jnp.where(left, total, 0.0), axis=1, keepdims=True)
    weight_sq = jnp.sum(jnp.where(left, 0.0, total), axis=1, keepdims=True)
    trust = jnp.sqrt(weight_sq) / jnp.sqrt(update_sq + 1e-06)
    factor = rate * trust
    out = []
    for p in range(pieces):
        span = pl.ds(p * height, height)
        fresh[span, :] = weight[span, :] - factor * update[span, :]
        copy = pltpu.make_async_copy(
            fresh.at[span], weight_out.at[span], piece_sem.at[p]
        )
        copy.start()
        out.append(copy)
    for copy in copies + out:
        copy.wait()


def local(grid, weights, moment, second, tile_rows, row_index, bucket_count):
    Z, L, X, C = grid
    n = Z * L * X * C
    rows_here, width = weights.shape
    slots = row_index.shape[0]
    capacity = slots // n
    groups = width // LANES
    pack = 8 // capacity
    tiles = tile_rows.reshape(n // pack, pack, capacity, groups, LANES)
    tiles = tiles.transpose(0, 3, 1, 2, 4)
    table = (rows_here, width)
    anywhere = pl.BlockSpec(memory_space=pl.ANY)
    outside = pl.BlockSpec(memory_space=pltpu.HBM)
    inside = pl.BlockSpec(memory_space=pltpu.VMEM)
    f32 = jnp.float32
    dma = pltpu.SemaphoreType.DMA
    held = pltpu.VMEM(table, f32)
    weight_v, moment_v, second_v, update_v, sums = pl.pallas_call(
        functools.partial(exchange, grid),
        out_shape=[jax.ShapeDtypeStruct(table, f32)] * 4
        + [jax.ShapeDtypeStruct((1, LANES), f32)],
        in_specs=[outside] * 6,
        out_specs=[inside] * 5,
        scratch_shapes=[
            pltpu.VMEM(tiles.shape, jnp.bfloat16),
            pltpu.VMEM((groups, n, capacity, LANES), jnp.bfloat16),
            pltpu.VMEM((L * X * C, Z, 1, slots), jnp.int32),
            pltpu.VMEM((L * X * C, Z, 1, n), jnp.int32),
            pltpu.VMEM((n, 1, LANES), f32),
            pltpu.VMEM((rows_here, slots), jnp.bfloat16),
            held, held, held,
            dma((3,)), dma((3,)), dma, pltpu.SemaphoreType.REGULAR,
            dma, dma, dma, dma((len(pieces_of(groups)),)),
            dma((2,)), dma((2,)), dma((2,)), dma((2,)), dma, dma,
        ],
        compiler_params=pltpu.CompilerParams(
            collective_id=0, has_side_effects=True, vmem_limit_bytes=36 * 1024 * 1024
        ),
        name="exchange",
    )(*(
        pltpu.with_memory_space_constraint(x, pltpu.HBM)
        for x in (
            weights, moment, second, tiles,
            row_index.reshape(1, slots), bucket_count.reshape(1, n),
        )
    ))
    pieces = 6
    return tuple(pl.pallas_call(
        finish,
        out_shape=[jax.ShapeDtypeStruct(table, f32)] * 3,
        in_specs=[inside] * 5,
        out_specs=[anywhere] * 3,
        scratch_shapes=[held, dma((2,)), dma((pieces,))],
        compiler_params=pltpu.CompilerParams(vmem_limit_bytes=24 * 1024 * 1024),
        name="finish",
    )(weight_v, moment_v, second_v, update_v, sums))


def solution(mesh):
    grid = factors(mesh.shape["rows"], mesh.shape["dp"])
    rows, flat = P(AXES, None), P(AXES)
    return jax.shard_map(
        functools.partial(local, grid),
        mesh=mesh,
        in_specs=(rows, rows, rows, rows, flat, flat),
        out_specs=(rows, rows, rows),
        check_vma=False,
    )
```

```python
import functools

import jax
import jax.numpy as jnp
from jax import lax
from jax.experimental import pallas as pl
from jax.experimental.pallas import tpu as pltpu
from jax.sharding import PartitionSpec as P

beta_one = 0.9
beta_two = 0.999
epsilon = 1e-06
decay = 0.01
rate = 0.1

AXES = ("rows", "dp")
LANES = 128


def factors(rows, dp):
    lo = max(d for d in range(1, rows + 1) if rows % d == 0 and d * d <= rows)
    core = 2 if dp % 2 == 0 else 1
    return rows // lo, lo, dp // core, core


def pieces_of(groups):
    small = groups // 4
    half = (groups - small) // 2
    sizes = [size for size in (small, half, groups - small - half) if size]
    return sizes


def exchange(
    grid, weights, moment, second, tiles, index, count,
    weight_out, moment_out, second_out, update_out, sums_out,
    staged, landed, index_all, count_all, weight_all, parts, picker, moment_in, second_in, decayed,
    load_sem, stage_sem, own_sem, ready, tile_send, near_recv, far_recv, chunk_recv,
    line_send, line_recv, plane_send, plane_recv, part_send, part_recv,
):
    Z, L, X, C = grid
    n = Z * L * X * C
    fast = X * C
    columns = L * X * C
    row_id, dp_id = lax.axis_index("rows"), lax.axis_index("dp")
    me = row_id * fast + dp_id
    hi, lo = row_id // L, lax.rem(row_id, L)
    x, core = dp_id // C, lax.rem(dp_id, C)
    column = lo * fast + dp_id
    rows_here, width = weights.shape
    groups = width // LANES
    slots = index.shape[-1]
    capacity = slots // n
    pack = tiles.shape[2]
    sizes = pieces_of(groups)

    half = Z // 2 if Z % 2 == 0 else 0
    if half:
        side = hi // half
        inside = hi - side * half
        line = [side * k + (1 - side) * (Z - 1 - k) for k in range(half)]
        line += [side * half + lax.rem(inside + j, half) for j in range(1, half)]
    else:
        line = [lax.rem(hi + j, Z) for j in range(1, Z)]
    los = [lo] + [lax.rem(lo + j, L) for j in range(1, L)]
    xs = [x] + [lax.rem(x + j, X) for j in range(1, X)]
    cores = [core] + [lax.rem(core + j, C) for j in range(1, C)]

    def spot(h, a, b, c):
        r, d = h * L + a, b * C + c
        return {"rows": r, "dp": d}, r * fast + d

    others = [
        (a, b, c)
        for c in cores
        for j, a in list(enumerate(los))[::-1]
        for k, b in list(enumerate(xs))[::-1]
        if j or k
    ]
    line_peers = [spot(h, lo, x, core) for h in line]
    plane_peers = [spot(hi, a, b, c) for a, b, c in others]
    plane_peers += [spot(hi, lo, x, c) for c in cores[1:]]
    near = [spot(h, lo, x, c) for h in line for c in cores] + plane_peers
    cross = [spot(h, a, b, c) for h in line[:half] for a, b, c in others]
    beside = [spot(h, a, b, c) for h in line[half:] for a, b, c in others]

    def mesh_copy(src, dst, send, recv, where):
        return pltpu.make_async_remote_copy(
            src_ref=src, dst_ref=dst, send_sem=send, recv_sem=recv,
            device_id=where, device_id_type=pl.DeviceIdType.MESH,
        )

    def drain(ref, sem):
        pltpu.make_async_copy(ref, ref, sem).wait()

    def send_rows(peers, start, size, recv):
        span = pl.ds(start, size)
        for where, peer in peers:
            mesh_copy(
                staged.at[peer // pack, span, lax.rem(peer, pack)],
                landed.at[span, me], tile_send, recv, where,
            ).start()

    stage = [
        pltpu.make_async_copy(tiles, staged, stage_sem.at[0]),
        pltpu.make_async_copy(index, index_all.at[column, hi], stage_sem.at[1]),
        pltpu.make_async_copy(count, count_all.at[column, hi], stage_sem.at[2]),
    ]
    for copy in stage:
        copy.start()
    barrier = pltpu.get_barrier_semaphore()
    for where, _ in near:
        pl.semaphore_signal(
            barrier, inc=1, device_id=where, device_id_type=pl.DeviceIdType.MESH
        )
    own = pltpu.make_async_copy(
        tiles.at[me // pack, :, lax.rem(me, pack)], landed.at[:, me], own_sem
    )
    own.start()
    loads = [
        pltpu.make_async_copy(weights, weight_out, load_sem.at[0]),
        pltpu.make_async_copy(moment, moment_in, load_sem.at[1]),
        pltpu.make_async_copy(second, second_in, load_sem.at[2]),
    ]
    for copy in stage:
        copy.wait()
    for load in loads:
        load.start()
    pl.semaphore_wait(barrier, len(near))

    for where, _ in line_peers:
        pl.semaphore_signal(
            ready, inc=1, device_id=where, device_id_type=pl.DeviceIdType.MESH
        )
    small = (index_all, count_all)
    for k, ref in enumerate(small):
        mine = ref.at[column, hi]
        for where, _ in line_peers:
            mesh_copy(mine, mine, line_send.at[k], line_recv.at[k], where).start()
    send_rows(near, 0, groups, near_recv)

    if line_peers:
        pl.semaphore_wait(ready, len(line_peers))
    end = (hi == 0) | (hi == Z - 1)
    inner = jnp.logical_not(end)
    aside = len(others)

    def send_chunks(peers):
        for q, size in enumerate(sizes):
            send_rows(peers, sum(sizes[:q]), size, chunk_recv.at[q])

    if half:
        pl.when(end)(lambda: send_rows(cross, 0, groups, far_recv))
        if half > 1:
            pl.when(inner)(lambda: send_rows(beside + cross[:aside], 0, groups, far_recv))

    else:
        send_rows(beside, 0, groups, far_recv)
    for k, ref in enumerate(small):
        if line_peers:
            drain(ref.at[column, pl.ds(0, Z - 1)], line_recv.at[k])
        block = ref.at[column]
        for where, _ in plane_peers:
            mesh_copy(block, block, plane_send.at[k], plane_recv.at[k], where).start()
    if half > 1:
        pl.when(end)(lambda: send_chunks(beside))
        pl.when(inner)(lambda: send_chunks(cross[aside:]))

    loads[0].wait()

    def columns_of(g):
        return pl.ds(pl.multiple_of(g * LANES, LANES), LANES)

    def weight_step(g, total):
        w = weight_out[:, columns_of(g)]
        decayed[:, columns_of(g)] = decay * w
        return total + jnp.sum((w * w).reshape(rows_here // 8, 8, LANES), axis=0)

    zero = jnp.zeros((8, LANES), jnp.float32)
    weight_sum = lax.fori_loop(0, groups, weight_step, zero, unroll=4)
    weight_row = jnp.sum(weight_sum, axis=0, keepdims=True)
    weight_all[column, hi] = weight_row
    mine = weight_all.at[column, hi]
    for where, _ in line_peers:
        mesh_copy(mine, mine, line_send.at[2], line_recv.at[2], where).start()

    loads[1].wait()
    loads[2].wait()

    @pl.loop(0, groups, unroll=4)
    def _(g):
        moment_in[:, columns_of(g)] = beta_one * moment_in[:, columns_of(g)]
        second_in[:, columns_of(g)] = beta_two * second_in[:, columns_of(g)]

    if plane_peers:
        for k, ref in enumerate(small):
            drain(ref.at[pl.ds(0, columns - 1)], plane_recv.at[k])
    index_rows = jnp.concatenate([index_all[:, h, 0, :] for h in range(Z)], axis=0)
    count_rows = jnp.concatenate([count_all[:, h, 0, :] for h in range(Z)], axis=0)
    lane = lax.broadcasted_iota(jnp.int32, (n, slots), 1)
    order = lax.broadcasted_iota(jnp.int32, (n, slots), 0)
    owner = lax.broadcasted_iota(jnp.int32, (n, n), 1)
    live = jnp.sum(jnp.where(owner == me, count_rows, 0), axis=1, keepdims=True)
    spread = jnp.zeros((n, slots), jnp.int32)
    for c in range(capacity):
        goal = jnp.sum(
            jnp.where(lane == me * capacity + c, index_rows, 0), axis=1, keepdims=True
        )
        goal = jnp.where(live > c, goal, -1)
        spread = spread + jnp.where(lane == order * capacity + c, goal, 0)
    target = jnp.sum(spread, axis=0, keepdims=True)
    row = lax.broadcasted_iota(jnp.int32, (rows_here, slots), 0)
    picker[...] = jnp.where(row == target, 1.0, 0.0).astype(jnp.bfloat16)

    own.wait()
    drain(landed.at[:, pl.ds(0, len(near))], near_recv)

    def arrived(start, size, from_end, from_inner, sem):
        def take(planes):
            if planes * aside:
                drain(landed.at[pl.ds(start, size), pl.ds(0, planes * aside)], sem)

        if half > 1:
            pl.when(end)(lambda: take(from_end))
            pl.when(inner)(lambda: take(from_inner))
        else:
            take(from_end)

    arrived(0, groups, 2 * half - 1 if half else Z - 1, half - 1, far_recv)

    if line_peers:
        drain(weight_all.at[column, pl.ds(0, Z - 1)], line_recv.at[2])
    block = weight_all.at[column]
    for where, _ in plane_peers:
        mesh_copy(block, block, plane_send.at[2], plane_recv.at[2], where).start()

    def step(g, total):
        cols = columns_of(g)
        block = landed[g].reshape(slots, LANES)
        gradient = jnp.dot(picker[...], block, preferred_element_type=jnp.float32)
        new_moment = moment_in[:, cols] + (1.0 - beta_one) * gradient
        new_second = second_in[:, cols] + (1.0 - beta_two) * gradient * gradient
        root = new_second * lax.rsqrt(new_second)
        update = new_moment / (root + epsilon) + decayed[:, cols]
        moment_out[:, cols] = new_moment
        second_out[:, cols] = new_second
        update_out[:, cols] = update
        return total + jnp.sum(
            (update * update).reshape(rows_here // 8, 8, LANES), axis=0
        )

    update_sum = zero
    start = 0
    for q, size in enumerate(sizes):
        arrived(start, size, 0, half, chunk_recv.at[q])
        update_sum = lax.fori_loop(
            start, start + size, step, update_sum, unroll=size
        )
        start += size

    update_row = jnp.sum(update_sum, axis=0, keepdims=True)
    parts[me] = update_row
    for where, _ in cross + beside + near:
        mesh_copy(parts.at[me], parts.at[me], part_send, part_recv, where).start()

    for k, ref in enumerate((*small, weight_all)):
        if line_peers:
            drain(ref.at[column, pl.ds(0, Z - 1)], line_send.at[k])
        if plane_peers:
            drain(ref.at[pl.ds(0, columns - 1)], plane_send.at[k])
    drain(landed.at[:, pl.ds(0, n - 1)], tile_send)
    if plane_peers:
        drain(weight_all.at[pl.ds(0, columns - 1)], plane_recv.at[2])
    sums_out[1:2] = jnp.sum(weight_all[...], axis=(0, 1))
    few = parts.at[pl.ds(0, n - 1)]
    drain(few, part_recv)
    sums_out[0:1] = jnp.sum(parts[...], axis=0)
    drain(few, part_send)


def finish(
    weight, moment, second, update, sums,
    weight_out, moment_out, second_out, fresh, sem, piece_sem,
):
    copies = [
        pltpu.make_async_copy(moment, moment_out, sem.at[0]),
        pltpu.make_async_copy(second, second_out, sem.at[1]),
    ]
    for copy in copies:
        copy.start()
    rows_here = weight.shape[0]
    pieces = piece_sem.shape[0]
    height = rows_here // pieces
    update_sq = jnp.sum(sums[0:1], axis=1, keepdims=True)
    weight_sq = jnp.sum(sums[1:2], axis=1, keepdims=True)
    trust = jnp.sqrt(weight_sq) / jnp.sqrt(update_sq + 1e-06)
    factor = rate * trust
    out = []
    for p in range(pieces):
        span = pl.ds(p * height, height)
        fresh[span, :] = weight[span, :] - factor * update[span, :]
        copy = pltpu.make_async_copy(
            fresh.at[span], weight_out.at[span], piece_sem.at[p]
        )
        copy.start()
        out.append(copy)
    for copy in copies + out:
        copy.wait()


def local(grid, weights, moment, second, tile_rows, row_index, bucket_count):
    Z, L, X, C = grid
    n = Z * L * X * C
    rows_here, width = weights.shape
    slots = row_index.shape[0]
    capacity = slots // n
    groups = width // LANES
    pack = 8 // capacity
    tiles = tile_rows.reshape(n // pack, pack, capacity, groups, LANES)
    tiles = tiles.transpose(0, 3, 1, 2, 4)
    table = (rows_here, width)
    anywhere = pl.BlockSpec(memory_space=pl.ANY)
    outside = pl.BlockSpec(memory_space=pltpu.HBM)
    inside = pl.BlockSpec(memory_space=pltpu.VMEM)
    f32 = jnp.float32
    dma = pltpu.SemaphoreType.DMA
    held = pltpu.VMEM(table, f32)
    weight_v, moment_v, second_v, update_v, sums = pl.pallas_call(
        functools.partial(exchange, grid),
        out_shape=[jax.ShapeDtypeStruct(table, f32)] * 4
        + [jax.ShapeDtypeStruct((2, LANES), f32)],
        in_specs=[outside] * 6,
        out_specs=[inside] * 5,
        scratch_shapes=[
            pltpu.VMEM(tiles.shape, jnp.bfloat16),
            pltpu.VMEM((groups, n, capacity, LANES), jnp.bfloat16),
            pltpu.VMEM((L * X * C, Z, 1, slots), jnp.int32),
            pltpu.VMEM((L * X * C, Z, 1, n), jnp.int32),
            pltpu.VMEM((L * X * C, Z, 1, LANES), f32),
            pltpu.VMEM((n, 1, LANES), f32),
            pltpu.VMEM((rows_here, slots), jnp.bfloat16),
            held, held, held,
            dma((3,)), dma((3,)), dma, pltpu.SemaphoreType.REGULAR,
            dma, dma, dma, dma((len(pieces_of(groups)),)),
            dma((3,)), dma((3,)), dma((3,)), dma((3,)), dma, dma,
        ],
        compiler_params=pltpu.CompilerParams(
            collective_id=0, has_side_effects=True, vmem_limit_bytes=36 * 1024 * 1024
        ),
        name="exchange",
    )(*(
        pltpu.with_memory_space_constraint(x, pltpu.HBM)
        for x in (
            weights, moment, second, tiles,
            row_index.reshape(1, slots), bucket_count.reshape(1, n),
        )
    ))
    pieces = 6
    return tuple(pl.pallas_call(
        finish,
        out_shape=[jax.ShapeDtypeStruct(table, f32)] * 3,
        in_specs=[inside] * 5,
        out_specs=[anywhere] * 3,
        scratch_shapes=[held, dma((2,)), dma((pieces,))],
        compiler_params=pltpu.CompilerParams(vmem_limit_bytes=24 * 1024 * 1024),
        name="finish",
    )(weight_v, moment_v, second_v, update_v, sums))


def solution(mesh):
    grid = factors(mesh.shape["rows"], mesh.shape["dp"])
    rows, flat = P(AXES, None), P(AXES)
    return jax.shard_map(
        functools.partial(local, grid),
        mesh=mesh,
        in_specs=(rows, rows, rows, rows, flat, flat),
        out_specs=(rows, rows, rows),
        check_vma=False,
    )
```
